32 devices in a mesh: dp: 16 (over z, y, core), inner: 2 (over x).
Axes of the slice: x: 2, y: 2, z: 4, core: 2. Of those that a mesh axis runs over, the one named last changes fastest.
Arguments:
- tokens: bfloat16 [65536, 768], P(('dp', 'inner')), may hold values from -6 to 6
- out_grad: bfloat16 [65536, 768], P(('dp', 'inner')), may hold values from -6 to 6
- norm1_gain: bfloat16 [768], P(('dp', 'inner')), may hold values from 0.5 to 1.5
- norm1_shift: bfloat16 [768], P(('dp', 'inner')), may hold values from -3 to 3
- qkv_weight: bfloat16 [768, 2304], P('dp', 'inner'), may hold values from -0.21875 to 0.21875
- qkv_bias: bfloat16 [2304], P(('dp', 'inner')), may hold values from -3 to 3
- proj_weight: bfloat16 [768, 768], P('dp', 'inner'), may hold values from -3 to 3
- proj_bias: bfloat16 [768], P(('dp', 'inner')), may hold values from -3 to 3
- norm2_gain: bfloat16 [768], P(('dp', 'inner')), may hold values from 0.5 to 1.5
- norm2_shift: bfloat16 [768], P(('dp', 'inner')), may hold values from -3 to 3
- up_weight: bfloat16 [768, 3072], P('dp', 'inner'), may hold values from -0.21875 to 0.21875
- up_bias: bfloat16 [3072], P(('dp', 'inner')), may hold values from -3 to 3
- down_weight: bfloat16 [3072, 768], P('dp', 'inner'), may hold values from -0.109375 to 0.109375
- down_bias: bfloat16 [768], P(('dp', 'inner')), may hold values from -3 to 3
Outputs:
- output: bfloat16 [65536, 768], P(('dp', 'inner'))
- grad_tokens: float32 [65536, 768], P(('dp', 'inner'))
- grad_norm1_gain: float32 [768], P(('dp', 'inner'))
- grad_norm1_shift: float32 [768], P(('dp', 'inner'))
- grad_qkv_weight: float32 [768, 2304], P('dp', 'inner')
- grad_qkv_bias: float32 [2304], P(('dp', 'inner'))
- grad_proj_weight: float32 [768, 768], P('dp', 'inner')
- grad_proj_bias: float32 [768], P(('dp', 'inner'))
- grad_norm2_gain: float32 [768], P(('dp', 'inner'))
- grad_norm2_shift: float32 [768], P(('dp', 'inner'))
- grad_up_weight: float32 [768, 3072], P('dp', 'inner')
- grad_up_bias: float32 [3072], P(('dp', 'inner'))
- grad_down_weight: float32 [3072, 768], P('dp', 'inner')
- grad_down_bias: float32 [768], P(('dp', 'inner'))
The draws below stay inside these ranges and needn't reach their ends.
All inputs are finite; a program needn't handle non-finite values.
Results may differ from the reference program's by a relative error of at most 0.02.
Values may be sent and summed in bfloat16 or wider, within the bound.
A program may use at most 256 MiB of HBM per device.

```python
import jax
import jax.numpy as jnp
from jax import lax

D = 768
HEADS = 12
HEAD_DIM = 64
FF = 3072
SHORT = 1024
LONG = 2048
TOK_DEV = 2048
TOKENS = 65536
N_DP = 16
N_INNER = 2


def shard_levels(own_key, extent, shards, least, largest):
    def one(dim, blocks):
        steps = jax.random.uniform(jax.random.fold_in(jax.random.fold_in(own_key, 6), dim), (blocks,), jnp.float32, least / len(shards), largest / len(shards))
        return jnp.repeat(jnp.exp(steps), extent[dim] // blocks).reshape((-1,) + (1,) * (len(extent) - dim - 1))

    gain = one(*shards[0])
    for cut in shards[1:]:
        gain = gain * one(*cut)
    return gain


def centred(key, dims, scale, bound, pieces=(), kind=jnp.bfloat16):
    gain = shard_levels(key, dims, pieces, -0.22, 0.18) if pieces else 1.0
    values = jax.random.normal(key, dims, jnp.float32) * scale * gain
    return jnp.minimum(jnp.maximum(values, -bound), bound).astype(kind)


def setup_inputs(seed: int = 0) -> dict:
    key_of = jax.random.split(jax.random.key(seed), 15)
    tokens = centred(key_of[0], (TOKENS, D), 1.0, 6.0, ((0, 32),))
    out_grad = centred(key_of[1], (TOKENS, D), 1.0, 6.0, ((0, 32),))
    norm1_gain = jnp.clip(1.0 + 0.1 * jax.random.normal(key_of[2], (D,), jnp.float32), 0.5, 1.5).astype(jnp.bfloat16)
    norm1_shift = centred(key_of[3], (D,), 0.5, 3.0, ((0, 32),))
    qkv_weight = centred(key_of[4], (D, 3 * D), D ** -0.5, 0.21875, ((0, 16), (1, 2)))
    qkv_bias = centred(key_of[5], (3 * D,), 0.5, 3.0, ((0, 32),))
    proj_weight = centred(key_of[6], (D, D), (D // 192) ** -0.5, 3.0, ((0, 16), (1, 2)))
    proj_bias = centred(key_of[7], (D,), 0.5, 3.0, ((0, 32),))
    norm2_gain = jnp.clip(1.0 + 0.1 * jax.random.normal(key_of[8], (D,), jnp.float32), 0.5, 1.5).astype(jnp.bfloat16)
    norm2_shift = centred(key_of[9], (D,), 0.5, 3.0, ((0, 32),))
    up_weight = centred(key_of[10], (D, FF), D ** -0.5, 0.21875, ((0, 16), (1, 2)))
    up_bias = centred(key_of[11], (FF,), 0.5, 3.0, ((0, 32),))
    down_weight = centred(key_of[12], (FF, D), FF ** -0.5, 0.109375, ((0, 16), (1, 2)))
    down_bias = centred(key_of[13], (D,), 0.5, 3.0, ((0, 32),))
    return {"tokens": tokens, "out_grad": out_grad, "norm1_gain": norm1_gain, "norm1_shift": norm1_shift, "qkv_weight": qkv_weight, "qkv_bias": qkv_bias, "proj_weight": proj_weight, "proj_bias": proj_bias, "norm2_gain": norm2_gain, "norm2_shift": norm2_shift, "up_weight": up_weight, "up_bias": up_bias, "down_weight": down_weight, "down_bias": down_bias}


@jax.custom_vjp
def low(v):
    return lax.optimization_barrier(v.astype(jnp.bfloat16)).astype(jnp.float32)

@jax.custom_vjp
def low_back(v):
    return v

def low_keep(v):
    return (low(v), None)

def low_pass(kept, grad):
    return (grad,)

def back_keep(v):
    return (v, None)

def back_low(kept, grad):
    return (low(grad),)
low.defvjp(low_keep, low_pass)
low_back.defvjp(back_keep, back_low)
highest = lax.Precision.HIGHEST

def layer_norm(values, gain_vec, shift_vec):
    center = values - lax.optimization_barrier(jnp.mean(values, axis=-1, keepdims=True))
    spread = lax.optimization_barrier(jnp.mean(center * center, axis=-1, keepdims=True))
    return center * lax.rsqrt(spread + 1e-05) * gain_vec + shift_vec

def attend_group(packed, group_index):
    seq_len = jnp.where(group_index // N_INNER < N_DP // 2, SHORT, LONG).astype(jnp.int32)
    split_heads = packed.reshape(TOK_DEV, 3, HEADS, HEAD_DIM)
    queries = split_heads[:, 0]
    keys_in = split_heads[:, 1]
    values_in = split_heads[:, 2]
    scores = low_back(jnp.einsum('qhd,khd->hqk', queries, keys_in, precision=highest) * HEAD_DIM ** (-0.5))
    row_pos = lax.broadcasted_iota(jnp.int32, (TOK_DEV, TOK_DEV), 0)
    col_pos = lax.broadcasted_iota(jnp.int32, (TOK_DEV, TOK_DEV), 1)
    allowed_mask = (col_pos <= row_pos) & (col_pos // seq_len == row_pos // seq_len)
    probabilities = jax.nn.softmax(jnp.where(allowed_mask, jnp.abs(scores), -1e+30), axis=-1)
    weights = low(jnp.sign(scores) * probabilities)
    attended = jnp.einsum('hqk,khd->qhd', weights, values_in, precision=highest)
    return attended.reshape(TOK_DEV, D)

def forward(tokens, parameters):
    gain_one, shift_one, qkv_weight, qkv_bias, proj_weight, proj_bias, gain_two, shift_two, up_weight, up_bias, down_weight, down_bias = parameters
    normed_one = low(layer_norm(tokens, gain_one, shift_one))
    packed = low_back(low(jnp.dot(normed_one, qkv_weight, precision=highest) + qkv_bias))
    groups = packed.reshape(-1, TOK_DEV, 3 * D)
    group_index = jnp.arange(groups.shape[0], dtype=jnp.int32)
    attended = lax.map(jax.checkpoint(lambda member: attend_group(member[0], member[1])), (groups, group_index))
    attended = low_back(low(attended.reshape(-1, D)))
    middle = tokens + low_back(jnp.dot(attended, proj_weight, precision=highest) + proj_bias)
    normed_two = low(layer_norm(middle, gain_two, shift_two))
    pre_act = low_back(jnp.dot(normed_two, up_weight, precision=highest) + up_bias)
    active = low(jax.nn.gelu(pre_act, approximate=True))
    return middle + jnp.dot(active, down_weight, precision=highest) + down_bias

def reference(tokens, out_grad, norm1_gain, norm1_shift, qkv_weight, qkv_bias, proj_weight, proj_bias, norm2_gain, norm2_shift, up_weight, up_bias, down_weight, down_bias):
    parameters = tuple((param.astype(jnp.float32) for param in (norm1_gain, norm1_shift, qkv_weight, qkv_bias, proj_weight, proj_bias, norm2_gain, norm2_shift, up_weight, up_bias, down_weight, down_bias)))
    result, pullback = jax.vjp(forward, tokens.astype(jnp.float32), parameters)
    grad_input, grads = pullback(out_grad.astype(jnp.float32))
    return (result.astype(jnp.bfloat16), grad_input, grads[0], grads[1], grads[2], grads[3], grads[4], grads[5], grads[6], grads[7], grads[8], grads[9], grads[10], grads[11])
```

```python
import functools
import jax, jax.numpy as jnp
from jax import lax
from jax.experimental import pallas as pl
from jax.experimental.pallas import tpu as pltpu

HD = 64
LOG2E = 1.4426950408889634
LN2 = 0.6931471805599453
BIG = 3.0e38
NT = (((1,), (1,)), ((), ()))
NN = (((1,), (0,)), ((), ()))
TN = (((0,), (0,)), ((), ()))


def dot(a, b, dims):
    return lax.dot_general(a, b, dims, preferred_element_type=jnp.float32)


def split_lanes(x):
    lane = lax.broadcasted_iota(jnp.int32, x.shape, 1)
    zero = jnp.zeros_like(x)
    return jnp.where(lane < HD, x, zero), jnp.where(lane < HD, zero, x)


def attn_fwd_kernel(B, C, seq_ref, q_ref, k_ref, v_ref, o_ref, lse_ref, vt_ref, acc_ref):
    rows = q_ref.shape[0]
    nb = rows // B
    vt_ref[...] = v_ref[...].T
    per = seq_ref[0] // B

    def q_loop(qb, _):
        q0 = pl.multiple_of(qb * B, B)
        q2 = split_lanes(q_ref[pl.ds(q0, B), :] * jnp.asarray(HD ** -0.5, jnp.bfloat16))

        def block(k0, width, mask, state):
            kb = k_ref[pl.ds(k0, width), :]
            new = []
            for h in range(2):
                m, l, acc = state[h]
                s = dot(kb, q2[h], NT)
                t = jnp.minimum(jnp.maximum(s * BIG, -LOG2E), LOG2E)
                a = s * t
                if mask is not None:
                    a = jnp.where(mask, a, -1e30)
                m1 = jnp.max(a, axis=0, keepdims=True)
                if m is not None:
                    m1 = jnp.maximum(m, m1)
                e = jnp.exp2(a - m1)
                l1 = jnp.sum(e, axis=0, keepdims=True)
                w = (t * e).astype(jnp.bfloat16)
                pv = dot(vt_ref[h * HD:(h + 1) * HD, pl.ds(k0, width)], w, NN)
                if m is not None:
                    alpha = jnp.exp2(m - m1)
                    l1 = l1 + alpha * l
                    pv = pv + alpha * acc
                new.append((m1, l1, pv))
            return tuple(new)

        ki = lax.broadcasted_iota(jnp.int32, (B, B), 0)
        qi = lax.broadcasted_iota(jnp.int32, (B, B), 1)
        state = block(q0, B, ki <= qi, ((None,) * 3,) * 2)
        first = (qb // per) * per

        def k_loop(j, st):
            return block(pl.multiple_of((first + j) * B, B), B, None, st)

        state = lax.fori_loop(0, qb - first, k_loop, state)
        outs = []
        for h in range(2):
            m, l, acc = state[h]
            outs.append(acc * (1.0 / (l * LOG2E)))
            lse_ref[0, h:h + 1, pl.ds(q0, B)] = m + jnp.log2(l * LOG2E)
        o_ref[pl.ds(q0, B), :] = jnp.concatenate(outs, axis=0).T.astype(jnp.bfloat16)
        return 0

    lax.fori_loop(0, nb, q_loop, 0)


def attn_fwd(packed, seq, B=256, pairs=6):
    rows = packed.shape[0]
    width = packed.shape[1] // 3
    n = width // 128
    spec = lambda off: pl.BlockSpec((rows, 128), lambda p, s: (0, off + p))
    return pl.pallas_call(
        functools.partial(attn_fwd_kernel, B, 0),
        out_shape=(jax.ShapeDtypeStruct((rows, width), jnp.bfloat16),
                   jax.ShapeDtypeStruct((n, 2, rows), jnp.float32)),
        grid_spec=pltpu.PrefetchScalarGridSpec(
            num_scalar_prefetch=1, grid=(n,),
            in_specs=[spec(0), spec(n), spec(2 * n)],
            out_specs=(pl.BlockSpec((rows, 128), lambda p, s: (0, p)),
                       pl.BlockSpec((1, 2, rows), lambda p, s: (p, 0, 0))),
            scratch_shapes=[pltpu.VMEM((128, rows), jnp.bfloat16), pltpu.VMEM((128, B), jnp.float32)]),
        name="attn_fwd",
    )(seq, packed, packed, packed)


def attn_bwd_kernel(B, seq_ref, q_ref, k_ref, v_ref, g_ref, o_ref, lse_ref, gq_ref, gk_ref, gv_ref,
                    kt_ref, gqt_ref, gk_acc, gv_acc, del_ref):
    rows = q_ref.shape[0]
    nb = rows // B
    kt_ref[...] = k_ref[...].T
    per = seq_ref[0] // B
    prod = g_ref[...].astype(jnp.float32) * o_ref[...].astype(jnp.float32)
    r8 = lax.broadcasted_iota(jnp.int32, (8, 128), 0)
    c8 = lax.broadcasted_iota(jnp.int32, (8, 128), 1)
    sel = jnp.where(r8 == c8 // HD, LN2, 0.0).astype(jnp.float32)
    del_ref[...] = lax.dot_general(sel, prod, NT, precision=lax.Precision.HIGHEST,
                                   preferred_element_type=jnp.float32)
    gqt_ref[...] = jnp.zeros_like(gqt_ref)

    ki = lax.broadcasted_iota(jnp.int32, (B, B), 0)
    qi = lax.broadcasted_iota(jnp.int32, (B, B), 1)
    tri = ki <= qi
    scale = jnp.asarray(HD ** -0.5, jnp.bfloat16)

    def k_loop(kb, _):
        k0 = pl.multiple_of(kb * B, B)
        kblk = k_ref[pl.ds(k0, B), :]
        vblk = v_ref[pl.ds(k0, B), :]
        last = (kb // per + 1) * per
        gk_acc[...] = jnp.zeros_like(gk_acc)
        gv_acc[...] = jnp.zeros_like(gv_acc)

        def block(qb, mask):
            q0 = pl.multiple_of(qb * B, B)
            q2 = split_lanes(q_ref[pl.ds(q0, B), :] * scale)
            g2 = split_lanes(g_ref[pl.ds(q0, B), :])
            gk = None
            for h in range(2):
                s = dot(kblk, q2[h], NT)
                dw = dot(vblk, g2[h], NT)
                t = jnp.minimum(jnp.maximum(s * BIG, -LOG2E), LOG2E)
                lse = lse_ref[0, h:h + 1, pl.ds(q0, B)]
                dl = del_ref[h:h + 1, pl.ds(q0, B)]
                e = jnp.exp2(s * t - lse)
                if mask is not None:
                    e = jnp.where(mask, e, 0.0)
                w = (t * e).astype(jnp.bfloat16)
                ds = (e * (dw - t * dl)).astype(jnp.bfloat16)
                gv_acc[...] += dot(w, g2[h], NN)
                gk_acc[...] += dot(ds, q2[h], NN)
                gqt_ref[h * HD:(h + 1) * HD, pl.ds(q0, B)] += dot(
                    kt_ref[h * HD:(h + 1) * HD, pl.ds(k0, B)], ds, NN)

        block(kb, tri)

        def q_loop(qb, c):
            block(qb, None)
            return c

        lax.fori_loop(kb + 1, last, q_loop, 0)
        gk_ref[pl.ds(k0, B), :] = (gk_acc[...] * LOG2E).astype(jnp.bfloat16)
        gv_ref[pl.ds(k0, B), :] = gv_acc[...].astype(jnp.bfloat16)
        return 0

    lax.fori_loop(0, nb, k_loop, 0)
    gq_ref[...] = (gqt_ref[...] * (LOG2E * HD ** -0.5)).T.astype(jnp.bfloat16)


def attn_bwd(packed, grad_att, att, lse, seq, B=256):
    rows = packed.shape[0]
    width = packed.shape[1] // 3
    n = width // 128
    spec = lambda off: pl.BlockSpec((rows, 128), lambda p, s: (0, off + p))
    out = jax.ShapeDtypeStruct((rows, width), jnp.bfloat16)
    return pl.pallas_call(
        functools.partial(attn_bwd_kernel, B),
        out_shape=(out, out, out),
        grid_spec=pltpu.PrefetchScalarGridSpec(
            num_scalar_prefetch=1, grid=(n,),
            in_specs=[spec(0), spec(n), spec(2 * n), spec(0), spec(0),
                      pl.BlockSpec((1, 2, rows), lambda p, s: (p, 0, 0))],
            out_specs=(spec(0), spec(0), spec(0)),
            scratch_shapes=[pltpu.VMEM((128, rows), jnp.bfloat16), pltpu.VMEM((128, rows), jnp.float32),
                            pltpu.VMEM((B, 128), jnp.float32), pltpu.VMEM((B, 128), jnp.float32),
                            pltpu.VMEM((8, rows), jnp.float32)]),
        name="attn_bwd",
    )(seq, packed, packed, packed, grad_att, att, lse)


from jax.sharding import PartitionSpec as P

SHORT = 1024
LONG = 2048
EPS = 1e-05
BOTH = ("inner", "dp")
F32 = jnp.float32
BF16 = jnp.bfloat16


def mm(a, b, dims=NN):
    return lax.dot_general(a, b, dims, preferred_element_type=F32)


def normalise(values):
    center = values - jnp.mean(values, axis=-1, keepdims=True)
    rs = lax.rsqrt(jnp.mean(center * center, axis=-1, keepdims=True) + EPS)
    return center * rs, rs


def norm_back(grad, n, rs, gain):
    t = grad * gain
    back = rs * (t - jnp.mean(t, axis=-1, keepdims=True) - n * jnp.mean(t * n, axis=-1, keepdims=True))
    return back, jnp.sum(grad * n, axis=0), jnp.sum(grad, axis=0)


def gelu(u):
    return jax.nn.gelu(u, approximate=True)


def gather_weight(shard):
    rows, cols = shard.shape
    n_in, n_dp = lax.axis_size("inner"), lax.axis_size("dp")
    got = lax.all_gather(shard, BOTH, axis=0, tiled=True)
    return got.reshape(n_in, n_dp * rows, cols).transpose(1, 0, 2).reshape(n_dp * rows, n_in * cols)


def scatter_weight(grad):
    n_in = lax.axis_size("inner")
    rows, cols = grad.shape
    laid = grad.astype(BF16).reshape(rows, n_in, cols // n_in).transpose(1, 0, 2)
    laid = laid.reshape(n_in * rows, cols // n_in)
    return lax.psum_scatter(laid, BOTH, scatter_dimension=0, tiled=True).astype(F32)


def pack_rows(parts, tile):
    flat = jnp.concatenate(parts, axis=-1)
    fill = -flat.shape[-1] % tile
    return jnp.pad(flat, [(0, 0)] * (flat.ndim - 1) + [(0, fill)])


def gather_vectors(vectors):
    sizes = [v.shape[0] for v in vectors]
    mine = pack_rows(vectors, 2048).reshape(-1, 128)
    got = lax.all_gather(mine, ("dp", "inner"), axis=0, tiled=True)
    n = lax.axis_size("dp") * lax.axis_size("inner")
    got = got.reshape(n, -1)
    out, at = [], 0
    for size in sizes:
        out.append(got[:, at:at + size].reshape(-1).astype(F32))
        at += size
    return out


def scatter_vectors(vectors):
    n = lax.axis_size("dp") * lax.axis_size("inner")
    parts = [v.reshape(n, -1) for v in vectors]
    sizes = [p.shape[1] for p in parts]
    laid = pack_rows(parts, 1024).reshape(-1, 128)
    got = lax.psum_scatter(laid, ("dp", "inner"), scatter_dimension=0, tiled=True).reshape(-1)
    out, at = [], 0
    for size in sizes:
        out.append(got[at:at + size])
        at += size
    return out


def on_device(tokens, out_grad, norm1_gain, norm1_shift, qkv_weight, qkv_bias, proj_weight, proj_bias,
              norm2_gain, norm2_shift, up_weight, up_bias, down_weight, down_bias):
    n_dp = lax.axis_size("dp")
    seq = jnp.where(lax.axis_index("dp") < n_dp // 2, SHORT, LONG).astype(jnp.int32).reshape(1)
    gain1, shift1, b_qkv, b_proj, gain2, shift2, b_up, b_down = gather_vectors(
        [norm1_gain, norm1_shift, qkv_bias, proj_bias, norm2_gain, norm2_shift, up_bias, down_bias])
    w_qkv = gather_weight(qkv_weight)
    w_proj = gather_weight(proj_weight)
    w_up = gather_weight(up_weight)
    w_down = gather_weight(down_weight)

    x = tokens.astype(F32)
    n1, r1 = normalise(x)
    h1 = (n1 * gain1 + shift1).astype(BF16)
    packed = (mm(h1, w_qkv) + b_qkv).astype(BF16)
    attended, lse = attn_fwd(packed, seq)
    middle = x + mm(attended, w_proj) + b_proj
    n2, r2 = normalise(middle)
    h2 = (n2 * gain2 + shift2).astype(BF16)
    pre = mm(h2, w_up) + b_up
    active = gelu(pre).astype(BF16)
    output = (middle + mm(active, w_down) + b_down).astype(BF16)

    e = out_grad.astype(F32)
    g_down_bias = jnp.sum(e, axis=0)
    g_active = mm(out_grad, w_down, NT)
    _, pull = jax.vjp(gelu, pre)
    g_pre = pull(g_active)[0].astype(BF16)
    g_down = mm(active, out_grad, TN).astype(BF16)
    g_up = mm(h2, g_pre, TN).astype(BF16)
    g_up_bias = jnp.sum(g_pre.astype(F32), axis=0)
    g_h2 = mm(g_pre, w_up, NT)
    back2, g_gain2, g_shift2 = norm_back(g_h2, n2, r2, gain2)
    g_middle = e + back2
    g_z = g_middle.astype(BF16)
    g_proj_bias = jnp.sum(g_z.astype(F32), axis=0)
    g_proj = mm(attended, g_z, TN).astype(BF16)
    g_att = mm(g_z, w_proj, NT).astype(BF16)
    g_att, g_up, g_down, g_proj = lax.optimization_barrier((g_att, g_up, g_down, g_proj))
    s_down = scatter_weight(g_down)
    s_up = scatter_weight(g_up)
    s_proj = scatter_weight(g_proj)

    g_packed = jnp.concatenate(attn_bwd(packed, g_att, attended, lse, seq), axis=1)
    g_qkv = mm(h1, g_packed, TN).astype(BF16)
    g_qkv_bias = jnp.sum(g_packed.astype(F32), axis=0)
    s_qkv = scatter_weight(g_qkv)
    g_h1 = mm(g_packed, w_qkv, NT)
    back1, g_gain1, g_shift1 = norm_back(g_h1, n1, r1, gain1)
    grad_tokens = g_middle + back1
    v = scatter_vectors([g_gain1, g_shift1, g_qkv_bias, g_proj_bias, g_gain2, g_shift2, g_up_bias, g_down_bias])
    return (output, grad_tokens, v[0], v[1], s_qkv, v[2], s_proj, v[3], v[4], v[5], s_up, v[6], s_down, v[7])


def solution(mesh):
    rows = P(("dp", "inner"), None)
    vec = P(("dp", "inner"))
    mat = P("dp", "inner")
    params = (vec, vec, mat, vec, mat, vec) * 2
    return jax.shard_map(on_device, mesh=mesh, in_specs=(rows, rows) + params,
                         out_specs=(rows, rows) + params, check_vma=False)
```

```python
import functools
import jax, jax.numpy as jnp
from jax import lax
from jax.experimental import pallas as pl
from jax.experimental.pallas import tpu as pltpu

HD = 64
LOG2E = 1.4426950408889634
LN2 = 0.6931471805599453
BIG = 3.0e38
NT = (((1,), (1,)), ((), ()))
NN = (((1,), (0,)), ((), ()))
TN = (((0,), (0,)), ((), ()))


def dot(a, b, dims):
    return lax.dot_general(a, b, dims, preferred_element_type=jnp.float32)


def split_lanes(x):
    lane = lax.broadcasted_iota(jnp.int32, x.shape, 1)
    zero = jnp.zeros_like(x)
    return jnp.where(lane < HD, x, zero), jnp.where(lane < HD, zero, x)


def attn_fwd_kernel(B, seq_ref, q_ref, k_ref, v_ref, o_ref, lse_ref, vt_ref, acc_ref):
    rows = q_ref.shape[0]
    nb = rows // B
    vt_ref[...] = v_ref[...].T
    per = seq_ref[0] // B

    def q_loop(qb, _):
        q0 = pl.multiple_of(qb * B, B)
        q2 = split_lanes(q_ref[pl.ds(q0, B), :] * jnp.asarray(HD ** -0.5, jnp.bfloat16))

        def block(k0, width, mask, state):
            kb = k_ref[pl.ds(k0, width), :]
            new = []
            for h in range(2):
                m, l, acc = state[h]
                s = dot(kb, q2[h], NT)
                t = jnp.minimum(jnp.maximum(s * BIG, -LOG2E), LOG2E)
                a = s * t
                if mask is not None:
                    a = jnp.where(mask, a, -1e30)
                m1 = jnp.max(a, axis=0, keepdims=True)
                if m is not None:
                    m1 = jnp.maximum(m, m1)
                e = jnp.exp2(a - m1)
                l1 = jnp.sum(e, axis=0, keepdims=True)
                w = (t * e).astype(jnp.bfloat16)
                pv = dot(vt_ref[h * HD:(h + 1) * HD, pl.ds(k0, width)], w, NN)
                if m is not None:
                    alpha = jnp.exp2(m - m1)
                    l1 = l1 + alpha * l
                    pv = pv + alpha * acc
                new.append((m1, l1, pv))
            return tuple(new)

        ki = lax.broadcasted_iota(jnp.int32, (B, B), 0)
        qi = lax.broadcasted_iota(jnp.int32, (B, B), 1)
        state = block(q0, B, ki <= qi, ((None,) * 3,) * 2)
        first = (qb // per) * per

        def k_loop(j, st):
            return block(pl.multiple_of((first + j) * B, B), B, None, st)

        state = lax.fori_loop(0, qb - first, k_loop, state)
        outs = []
        for h in range(2):
            m, l, acc = state[h]
            outs.append(acc * (1.0 / (l * LOG2E)))
            lse_ref[0, h:h + 1, pl.ds(q0, B)] = m + jnp.log2(l * LOG2E)
        o_ref[pl.ds(q0, B), :] = jnp.concatenate(outs, axis=0).T.astype(jnp.bfloat16)
        return 0

    lax.fori_loop(0, nb, q_loop, 0)


def attn_fwd(packed, seq, B=512):
    rows = packed.shape[0]
    width = packed.shape[1] // 3
    n = width // 128
    spec = lambda off: pl.BlockSpec((rows, 128), lambda p, s: (0, off + p))
    return pl.pallas_call(
        functools.partial(attn_fwd_kernel, B),
        out_shape=(jax.ShapeDtypeStruct((rows, width), jnp.bfloat16),
                   jax.ShapeDtypeStruct((n, 2, rows), jnp.float32)),
        grid_spec=pltpu.PrefetchScalarGridSpec(
            num_scalar_prefetch=1, grid=(n,),
            in_specs=[spec(0), spec(n), spec(2 * n)],
            out_specs=(pl.BlockSpec((rows, 128), lambda p, s: (0, p)),
                       pl.BlockSpec((1, 2, rows), lambda p, s: (p, 0, 0))),
            scratch_shapes=[pltpu.VMEM((128, rows), jnp.bfloat16), pltpu.VMEM((128, B), jnp.float32)]),
        name="attn_fwd",
    )(seq, packed, packed, packed)


def attn_bwd_kernel(B, seq_ref, q_ref, k_ref, v_ref, g_ref, o_ref, lse_ref, gq_ref, gk_ref, gv_ref,
                    kt_ref, gqt_ref, gk_acc, gv_acc, del_ref):
    rows = q_ref.shape[0]
    nb = rows // B
    kt_ref[...] = k_ref[...].T
    per = seq_ref[0] // B
    prod = g_ref[...].astype(jnp.float32) * o_ref[...].astype(jnp.float32)
    r8 = lax.broadcasted_iota(jnp.int32, (8, 128), 0)
    c8 = lax.broadcasted_iota(jnp.int32, (8, 128), 1)
    sel = jnp.where(r8 == c8 // HD, LN2, 0.0).astype(jnp.float32)
    del_ref[...] = lax.dot_general(sel, prod, NT, precision=lax.Precision.HIGHEST,
                                   preferred_element_type=jnp.float32)
    gqt_ref[...] = jnp.zeros_like(gqt_ref)

    ki = lax.broadcasted_iota(jnp.int32, (B, B), 0)
    qi = lax.broadcasted_iota(jnp.int32, (B, B), 1)
    tri = ki <= qi
    scale = jnp.asarray(HD ** -0.5, jnp.bfloat16)

    def k_loop(kb, _):
        k0 = pl.multiple_of(kb * B, B)
        kblk = k_ref[pl.ds(k0, B), :]
        vblk = v_ref[pl.ds(k0, B), :]
        last = (kb // per + 1) * per
        gk_acc[...] = jnp.zeros_like(gk_acc)
        gv_acc[...] = jnp.zeros_like(gv_acc)

        def block(qb, mask):
            q0 = pl.multiple_of(qb * B, B)
            q2 = split_lanes(q_ref[pl.ds(q0, B), :] * scale)
            g2 = split_lanes(g_ref[pl.ds(q0, B), :])
            for h in range(2):
                s = dot(kblk, q2[h], NT)
                dw = dot(vblk, g2[h], NT)
                t = jnp.minimum(jnp.maximum(s * BIG, -LOG2E), LOG2E)
                lse = lse_ref[0, h:h + 1, pl.ds(q0, B)]
                dl = del_ref[h:h + 1, pl.ds(q0, B)]
                e = jnp.exp2(s * t - lse)
                if mask is not None:
                    e = jnp.where(mask, e, 0.0)
                w = (t * e).astype(jnp.bfloat16)
                ds = (e * (dw - t * dl)).astype(jnp.bfloat16)
                gv_acc[...] += dot(w, g2[h], NN)
                gk_acc[...] += dot(ds, q2[h], NN)
                gqt_ref[h * HD:(h + 1) * HD, pl.ds(q0, B)] += dot(
                    kt_ref[h * HD:(h + 1) * HD, pl.ds(k0, B)], ds, NN)

        block(kb, tri)

        def q_loop(qb, c):
            block(qb, None)
            return c

        lax.fori_loop(kb + 1, last, q_loop, 0)
        gk_ref[pl.ds(k0, B), :] = (gk_acc[...] * LOG2E).astype(jnp.bfloat16)
        gv_ref[pl.ds(k0, B), :] = gv_acc[...].astype(jnp.bfloat16)
        return 0

    lax.fori_loop(0, nb, k_loop, 0)
    gq_ref[...] = (gqt_ref[...] * (LOG2E * HD ** -0.5)).T.astype(jnp.bfloat16)


def attn_bwd(packed, grad_att, att, lse, seq, B=512):
    rows = packed.shape[0]
    width = packed.shape[1] // 3
    n = width // 128
    spec = lambda off: pl.BlockSpec((rows, 128), lambda p, s: (0, off + p))
    out = jax.ShapeDtypeStruct((rows, width), jnp.bfloat16)
    return pl.pallas_call(
        functools.partial(attn_bwd_kernel, B),
        out_shape=(out, out, out),
        grid_spec=pltpu.PrefetchScalarGridSpec(
            num_scalar_prefetch=1, grid=(n,),
            in_specs=[spec(0), spec(n), spec(2 * n), spec(0), spec(0),
                      pl.BlockSpec((1, 2, rows), lambda p, s: (p, 0, 0))],
            out_specs=(spec(0), spec(0), spec(0)),
            scratch_shapes=[pltpu.VMEM((128, rows), jnp.bfloat16), pltpu.VMEM((128, rows), jnp.float32),
                            pltpu.VMEM((B, 128), jnp.float32), pltpu.VMEM((B, 128), jnp.float32),
                            pltpu.VMEM((8, rows), jnp.float32)]),
        name="attn_bwd",
    )(seq, packed, packed, packed, grad_att, att, lse)


from jax.sharding import PartitionSpec as P


SHORT = 1024
LONG = 2048
EPS = 1e-05
BOTH = ("inner", "dp")
F32 = jnp.float32
BF16 = jnp.bfloat16


def mm(a, b, dims=NN):
    return lax.dot_general(a, b, dims, preferred_element_type=F32)


def normalise(values):
    center = values - jnp.mean(values, axis=-1, keepdims=True)
    rs = lax.rsqrt(jnp.mean(center * center, axis=-1, keepdims=True) + EPS)
    return center * rs, rs


def norm_back(grad, n, rs, gain):
    t = grad * gain
    back = rs * (t - jnp.mean(t, axis=-1, keepdims=True) - n * jnp.mean(t * n, axis=-1, keepdims=True))
    return back, jnp.sum(grad * n, axis=0), jnp.sum(grad, axis=0)


def gelu(u):
    return jax.nn.gelu(u, approximate=True)


def lay_vectors(parts, width):
    flat = jnp.concatenate(parts, axis=1).astype(BF16)
    fill = -flat.shape[1] % (16 * width)
    return jnp.pad(flat, ((0, 0), (0, fill))).reshape(flat.shape[0], -1, width)


def gather_all(weights, vectors, width):
    n_in, n_dp = lax.axis_size("inner"), lax.axis_size("dp")
    pieces, plan = [], []
    for w in weights:
        count = w.shape[1] // width
        plan.append((w.shape[0], count))
        pieces += [w[:, j * width:(j + 1) * width] for j in range(count)]
    if vectors:
        pieces.append(lay_vectors([v.reshape(1, -1) for v in vectors], width)[0])
    mine = jnp.concatenate(pieces, axis=0)
    got = lax.all_gather(mine, BOTH, axis=0, tiled=True).reshape(n_in, n_dp, mine.shape[0], width)
    whole, at = [], 0
    for rows, count in plan:
        cols = []
        for i in range(n_in):
            for j in range(count):
                lo = at + j * rows
                cols.append(got[i, :, lo:lo + rows].reshape(n_dp * rows, width))
        whole.append(jnp.concatenate(cols, axis=1))
        at += rows * count
    if not vectors:
        return whole, []
    flat = got[:, :, at:].transpose(1, 0, 2, 3).reshape(n_dp * n_in, -1)
    vecs, at = [], 0
    for v in vectors:
        vecs.append(flat[:, at:at + v.shape[0]].reshape(-1).astype(F32))
        at += v.shape[0]
    return whole, vecs


def lay_grads(grads, vectors, width):
    n_in, n_dp = lax.axis_size("inner"), lax.axis_size("dp")
    if vectors:
        vecs = lay_vectors([v.reshape(n_dp * n_in, -1) for v in vectors], width)
        vecs = vecs.reshape(n_dp, n_in, -1, width)
    halves = []
    for i in range(n_in):
        pieces = []
        for g in grads:
            part = g.shape[1] // n_in
            for j in range(part // width):
                lo = i * part + j * width
                pieces.append(g[:, lo:lo + width].reshape(n_dp, -1, width))
        if vectors:
            pieces.append(vecs[:, i])
        halves.append(jnp.concatenate(pieces, axis=1))
    laid = jnp.concatenate(halves, axis=0)
    return laid.reshape(-1, width)


def take_grads(mine, shapes, sizes, width):
    out, at = [], 0
    for rows, cols in shapes:
        count = cols // width
        out.append(jnp.concatenate([mine[at + j * rows:at + (j + 1) * rows] for j in range(count)], axis=1))
        at += rows * count
    flat = mine[at:].reshape(-1)
    vecs, at = [], 0
    for size in sizes:
        vecs.append(flat[at:at + size])
        at += size
    return [o.astype(F32) for o in out], [v.astype(F32) for v in vecs]


def scatter(laid):
    return lax.psum_scatter(laid, BOTH, scatter_dimension=0, tiled=True)


def on_device(tokens, out_grad, norm1_gain, norm1_shift, qkv_weight, qkv_bias, proj_weight, proj_bias,
              norm2_gain, norm2_shift, up_weight, up_bias, down_weight, down_bias):
    n_dp = lax.axis_size("dp")
    seq = jnp.where(lax.axis_index("dp") < n_dp // 2, SHORT, LONG).astype(jnp.int32).reshape(1)
    width = proj_weight.shape[1]
    vectors = [norm1_gain, norm1_shift, qkv_bias, proj_bias, norm2_gain, norm2_shift, up_bias, down_bias]
    (w_qkv,), vecs = gather_all([qkv_weight], vectors, width)
    gain1, shift1, b_qkv, b_proj, gain2, shift2, b_up, b_down = vecs
    (w_proj, w_up, w_down), _ = gather_all([proj_weight, up_weight, down_weight], [], width)

    x = tokens.astype(F32)
    n1, r1 = normalise(x)
    h1 = (n1 * gain1 + shift1).astype(BF16)
    packed = (mm(h1, w_qkv) + b_qkv).astype(BF16)
    attended, lse = attn_fwd(packed, seq)
    middle = x + mm(attended, w_proj) + b_proj
    n2, r2 = normalise(middle)
    h2 = (n2 * gain2 + shift2).astype(BF16)
    pre = mm(h2, w_up) + b_up
    active = gelu(pre).astype(BF16)
    output = (middle + mm(active, w_down) + b_down).astype(BF16)

    e = out_grad.astype(F32)
    g_down_bias = jnp.sum(e, axis=0)
    g_active = mm(out_grad, w_down, NT)
    _, pull = jax.vjp(gelu, pre)
    g_pre = pull(g_active)[0].astype(BF16)
    g_down = mm(active, out_grad, TN).astype(BF16)
    g_up = mm(h2, g_pre, TN).astype(BF16)
    g_up_bias = jnp.sum(g_pre.astype(F32), axis=0)
    g_h2 = mm(g_pre, w_up, NT)
    back2, g_gain2, g_shift2 = norm_back(g_h2, n2, r2, gain2)
    g_middle = e + back2
    g_z = g_middle.astype(BF16)
    g_proj_bias = jnp.sum(g_z.astype(F32), axis=0)
    g_proj = mm(attended, g_z, TN).astype(BF16)
    g_att = mm(g_z, w_proj, NT).astype(BF16)
    laid = lay_grads([g_proj, g_up, g_down], [], width)
    g_att, laid = lax.optimization_barrier((g_att, laid))
    mine = scatter(laid)
    (s_proj, s_up, s_down), _ = take_grads(
        mine, [proj_weight.shape, up_weight.shape, down_weight.shape], [], width)

    g_packed = jnp.concatenate(attn_bwd(packed, g_att, attended, lse, seq), axis=1)
    g_qkv = mm(h1, g_packed, TN).astype(BF16)
    g_qkv_bias = jnp.sum(g_packed.astype(F32), axis=0)
    g_h1 = mm(g_packed, w_qkv, NT)
    back1, g_gain1, g_shift1 = norm_back(g_h1, n1, r1, gain1)
    grad_tokens = g_middle + back1
    g_vecs = [g_gain1, g_shift1, g_qkv_bias, g_proj_bias, g_gain2, g_shift2, g_up_bias, g_down_bias]
    laid = lay_grads([g_qkv], g_vecs, width)
    mine = scatter(laid)
    (s_qkv,), v = take_grads(mine, [qkv_weight.shape], [u.shape[0] for u in vectors], width)
    return (output, grad_tokens, v[0], v[1], s_qkv, v[2], s_proj, v[3], v[4], v[5], s_up, v[6], s_down, v[7])


def solution(mesh):
    rows = P(("dp", "inner"), None)
    vec = P(("dp", "inner"))
    mat = P("dp", "inner")
    params = (vec, vec, mat, vec, mat, vec) * 2

    return jax.shard_map(on_device, mesh=mesh, in_specs=(rows, rows) + params,
                         out_specs=(rows, rows) + params, check_vma=False)
```
